32 devices in a mesh: dom: 32 (over z, y, x, core).
Axes of the slice: x: 2, y: 2, z: 4, core: 2. Of those that a mesh axis runs over, the one named last changes fastest.
Arguments:
- field: float32 [3, 180224], P(None, 'dom'), may hold values from -6 to 6
- blocks: bfloat16 [30, 30, 131072], P(None, None, 'dom'), may hold values from -1 to 1
- connectivity: int32 [10, 131072], P(None, 'dom'), may hold values from 0 to 8703, as said below
- send_nodes: int32 [8, 12288], P(None, 'dom'), may hold values from 0 to 5631
- live_blocks: int32 [32], replicated, may hold values from 1 to 8
Outputs:
- image: float32 [3, 180224], P(None, 'dom')
The draws below stay inside these ranges and needn't reach their ends.
Inputs may be any that keep to these rules, and one draw needn't show every extreme that they name: `connectivity`: entries below 5632 name nodes of the element's own subdomain; entry 5632 + k * 384 + g names the node sent as entry g of row k by subdomain d - o_k, and only where that subdomain exists. `send_nodes`: columns d * 384 to (d + 1) * 384 - 1 of row k list local indices of nodes that subdomain d owns, in the order in which subdomain d + o_k numbers its ghost slots from d. Subdomain d's elements fill its first 512 * live_blocks[d] slots; the other slots are unused.
All inputs are finite; a program needn't handle non-finite values.
Results may differ from the reference program's by a relative error of at most 0.0003.
Values sent between devices are 32-bit elements; how exact they have to be, the bound alone decides.
A program may use at most 64 MiB of HBM per device.

```python
import jax
import jax.numpy as jnp
from jax import lax

ELEM_DEV = 4096
BLK = 512
REACH = 4
NODE_DEV = 5632
GHOST = 384
NBLK = 8
NODES = 180224
ELEMS = 131072
N_DOM = 32


def draw_connectivity(key, part):
    slot_total = N_DOM * ELEM_DEV
    key_local, key_ghost, key_pick = jax.random.split(jax.random.fold_in(key, 11), 3)
    local_ids = jax.random.randint(key_local, (10, slot_total), 0, NODE_DEV)
    ghost_ids = jax.random.randint(key_ghost, (10, slot_total), 0, 2 * REACH * GHOST)
    picked = jax.random.randint(key_pick, (10, slot_total), 0, 5) == 0
    device = jnp.arange(slot_total, dtype=jnp.int32)[None, :] // ELEM_DEV
    bucket = ghost_ids // GHOST
    offset = jnp.where(bucket < REACH, bucket + 1, REACH - 1 - bucket)
    source = device - offset
    usable = picked & (source >= 0) & (source < N_DOM)
    return jnp.where(usable, NODE_DEV + ghost_ids, local_ids).astype(jnp.int32)


def plant(values, key, low, high):
    spot = [jax.random.randint(jax.random.fold_in(key, axis), (), 0, length) for axis, length in enumerate(values.shape)]
    longest = values.shape.index(max(values.shape))
    beside = spot[:longest] + [(spot[longest] + 1) % values.shape[longest]] + spot[longest + 1:]
    return values.at[tuple(spot)].set(low).at[tuple(beside)].set(high)


def block_scale(stream_key, shape, cuts, smallest, high):
    factor_of, own = 1.0, jax.random.fold_in(stream_key, 6)
    for position, shards_of in cuts:
        steps = jnp.exp(jax.random.uniform(jax.random.fold_in(own, position), (shards_of,), jnp.float32, smallest / len(cuts), high / len(cuts)))
        factor_of = factor_of * jnp.repeat(steps, shape[position] // shards_of).reshape([-1 if axis == position else 1 for axis in range(len(shape))])
    return factor_of


def noise(stream_key, dims, scale, most, shards=(), kind=jnp.bfloat16):
    gain = block_scale(stream_key, dims, shards, -0.22, 0.18) if shards else 1.0
    drawn = jax.random.normal(stream_key, dims, jnp.float32) * scale * gain
    return jnp.minimum(jnp.maximum(drawn, -most), most).astype(kind)


def setup_inputs(seed: int = 0) -> dict:
    arg_keys = jax.random.split(jax.random.key(seed), 6)
    field = noise(arg_keys[0], (3, NODES), 1.0, 6.0, ((1, 32),), jnp.float32)
    blocks = noise(arg_keys[1], (30, 30, ELEMS), 30 ** -0.5, 1.0, ((2, 32),))
    connectivity = draw_connectivity(jax.random.fold_in(arg_keys[5], 71), 0)
    send_nodes = plant(jax.random.randint(arg_keys[3], (2 * REACH, N_DOM * GHOST), 0, NODE_DEV), jax.random.fold_in(arg_keys[3], 1), 0, NODE_DEV - 1).astype(jnp.int32)
    live_blocks = plant(jax.random.randint(arg_keys[4], (N_DOM,), NBLK // 8, NBLK + 1), jax.random.fold_in(arg_keys[4], 1), NBLK // 8, NBLK).astype(jnp.int32)
    return {"field": field, "blocks": blocks, "connectivity": connectivity, "send_nodes": send_nodes, "live_blocks": live_blocks}


def reference(field, blocks, connectivity, send_nodes, live_blocks):
    node_total = N_DOM * NODE_DEV
    offsets = jnp.array([k + 1 if k < REACH else REACH - 1 - k for k in range(2 * REACH)], jnp.int32)
    padded = jnp.concatenate([field, jnp.zeros((3, 1), field.dtype)], axis=1)

    def partition_step(totals, device):
        local_ids = device * NODE_DEV + jnp.arange(NODE_DEV, dtype=jnp.int32)
        pieces = [local_ids]
        for k in range(2 * REACH):
            source = device - offsets[k]
            inside = (source >= 0) & (source < N_DOM)
            clipped = jnp.clip(source, 0, N_DOM - 1).astype(jnp.int32)
            sent_rows = lax.dynamic_slice_in_dim(send_nodes[k], clipped * GHOST, GHOST)
            pieces.append(jnp.where(inside, clipped * NODE_DEV + sent_rows, node_total).astype(jnp.int32))
        global_ids = jnp.concatenate(pieces)
        element_nodes = lax.dynamic_slice_in_dim(connectivity, (device * ELEM_DEV).astype(jnp.int32), ELEM_DEV, 1)
        node_ids = global_ids[element_nodes]
        values = padded[:, node_ids].reshape(30, ELEM_DEV)
        stiffness = lax.dynamic_slice_in_dim(blocks, (device * ELEM_DEV).astype(jnp.int32), ELEM_DEV, 2).astype(jnp.float32)
        forces = jnp.einsum("ije,je->ie", stiffness, values, precision=lax.Precision.HIGHEST)
        live_mask = jnp.arange(ELEM_DEV, dtype=jnp.int32) < live_blocks[device] * BLK
        forces = jnp.where(live_mask[None, :], forces, 0.0)
        totals = totals.at[:, node_ids.reshape(-1)].add(forces.reshape(3, 10 * ELEM_DEV))
        return totals, None

    totals = jnp.zeros((3, node_total + 1), jnp.float32)
    totals, _ = lax.scan(partition_step, totals, jnp.arange(N_DOM, dtype=jnp.int32))
    return totals[:, :node_total]
```

```python
import functools

import jax
import jax.numpy as jnp
from jax import lax
from jax.experimental import pallas as pl
from jax.experimental.pallas import tpu as pltpu
from jax.sharding import PartitionSpec as P

BLK = 512
LANES = 128
WIDE = 256
MESH = pl.DeviceIdType.MESH
VM = pl.BlockSpec(memory_space=pltpu.VMEM)
BF = jnp.bfloat16


def round_up(n, m):
    return -(-n // m) * m


def split_parts(x):
    high = x.astype(BF)
    low = (x - high.astype(jnp.float32)).astype(BF)
    return high, low


def narrow(x):
    return x.astype(jnp.float32).astype(BF)


def row_numbers(height, width):
    return narrow(lax.broadcasted_iota(jnp.int32, (height, width), 0))


def lane_hot(indices):
    lower = narrow(jnp.bitwise_and(indices, LANES - 1))
    return jnp.where(row_numbers(LANES, indices.shape[1]) == lower, BF(1), BF(0))


def pick(table, hot, upper, height):
    spread = jnp.dot(
        table, jnp.concatenate([hot, hot], axis=0), preferred_element_type=jnp.float32
    )
    sub = lax.broadcasted_iota(jnp.int32, (8, upper.shape[1]), 0)
    masks = [sub == upper - u for u in range(0, height, 8)]
    rows = []
    for c in range(3):
        found = jnp.zeros(sub.shape, jnp.float32)
        for t, mask in enumerate(masks):
            at = c * height + 8 * t
            found = jnp.where(mask, spread[at:at + 8], found)
        rows.append(jnp.sum(found, axis=0, keepdims=True))
    return rows


def spread_back(rows, hot, indices, height):
    seg = jnp.right_shift(indices, 7)
    bit = narrow(jnp.bitwise_and(seg, 1))
    upper = narrow(jnp.right_shift(seg, 1))
    zero = BF(0)
    wide = jnp.concatenate(
        [jnp.where(bit == zero, hot, zero), jnp.where(bit == zero, zero, hot)], axis=0
    )
    width = indices.shape[1]
    total = 2 * height
    r = lax.broadcasted_iota(jnp.int32, (total, width), 0)
    mask = narrow(jnp.where(r >= height, r - height, r)) == upper
    first, last = height // 16 * 16, round_up(height, 16)
    pieces = []
    for row in rows:
        high, low = split_parts(row)
        pieces.append(jnp.where(mask[:first], high, zero))
        if last > first:
            middle = jnp.where(row_numbers(last - first, width) < BF(height - first), high, low)
            pieces.append(jnp.where(mask[first:last], middle, zero))
        pieces.append(jnp.where(mask[last:], low, zero))
    placed = jnp.concatenate(pieces, axis=0)
    return lax.dot_general(
        placed, wide, (((1,), (1,)), ((), ())), preferred_element_type=jnp.float32
    )


def kernel(
    devices, offsets, live_ref, field_ref, send_ref, conn_ref, blocks_hbm, out_ref,
    tabf, table, outgoing, ghosts, back, returned, sent_hot, hots, values, v_ref, f_ref, total,
    blocks, block_sem, send_sem, recv_sem, back_sem, ret_sem,
):
    me = lax.axis_index("dom")
    nodes = field_ref.shape[1]
    reach, bucket = send_ref.shape
    corners, elements = conn_ref.shape
    steps = elements // BLK
    local_height = table.shape[0] // 3
    all_height = total.shape[0] // 6

    def inside(k, sign):
        other = me + sign * offsets[k]
        return (other >= 0) & (other < devices)

    barrier = pltpu.get_barrier_semaphore()
    count = 0
    for k in range(reach):
        count = count + inside(k, 1).astype(jnp.int32)

        @pl.when(inside(k, 1))
        def _():
            pl.semaphore_signal(
                barrier, inc=1, device_id=(me + offsets[k],), device_id_type=MESH
            )

    def block_copy(b):
        return pltpu.make_async_copy(
            blocks_hbm.at[:, :, pl.ds(pl.multiple_of(b * BLK, BLK), BLK)],
            blocks.at[b],
            block_sem.at[b],
        )

    for b in range(steps):
        block_copy(b).start()

    tabf[...] = jnp.zeros_like(tabf)
    for c in range(3):
        for t in range(nodes // LANES):
            row = c * local_height + t
            tabf[row:row + 1, :] = field_ref[c:c + 1, t * LANES:(t + 1) * LANES]
    high, low = split_parts(tabf[...])
    table[:, :LANES] = high
    table[:, LANES:] = low

    for k in range(reach):
        indices = send_ref[k:k + 1, :]
        hot = lane_hot(indices)
        sent_hot[k] = hot
        rows = pick(table[...], hot, jnp.right_shift(indices, 7), local_height)
        for c in range(3):
            outgoing[k, c:c + 1, :] = rows[c]

    pl.semaphore_wait(barrier, count)

    def out_copy(k):
        return pltpu.make_async_remote_copy(
            src_ref=outgoing.at[k], dst_ref=ghosts.at[k],
            send_sem=send_sem.at[k], recv_sem=recv_sem.at[k],
            device_id=(me + offsets[k],), device_id_type=MESH,
        )

    def back_copy(k):
        return pltpu.make_async_remote_copy(
            src_ref=back.at[k], dst_ref=returned.at[k],
            send_sem=back_sem.at[k], recv_sem=ret_sem.at[k],
            device_id=(me - offsets[k],), device_id_type=MESH,
        )

    order = sorted(range(reach), key=lambda k: -abs(offsets[k]))
    for k in order:

        @pl.when(inside(k, 1))
        def _():
            out_copy(k).start()

    for k in range(reach):

        @pl.when(jnp.logical_not(inside(k, -1)))
        def _():
            ghosts[k] = jnp.zeros(ghosts.shape[1:], jnp.float32)

        @pl.when(jnp.logical_not(inside(k, 1)))
        def _():
            returned[k] = jnp.zeros(returned.shape[1:], jnp.float32)

    total[...] = jnp.zeros_like(total)

    def local_step(b, _):
        at = pl.ds(pl.multiple_of(b * BLK, BLK), BLK)
        for a in range(corners):
            indices = conn_ref[a:a + 1, at]
            hot = lane_hot(indices)
            hots[b * corners + a] = hot
            rows = pick(table[...], hot, jnp.right_shift(indices, 7), local_height)
            for c in range(3):
                values[b, c * 16 + a:c * 16 + a + 1, :] = rows[c]
        return 0

    lax.fori_loop(0, steps, local_step, 0)

    for k in order:

        @pl.when(inside(k, 1))
        def _():
            out_copy(k).wait_send()

        @pl.when(inside(k, -1))
        def _():
            out_copy(k).wait_recv()

    live = live_ref[me]
    segs = bucket // LANES
    rest = corners - 8
    groups = BLK // LANES

    def element_step(b, _):
        at = pl.ds(pl.multiple_of(b * BLK, BLK), BLK)
        index = conn_ref[:, at]
        beyond = index - nodes
        shifts = jnp.right_shift(beyond, 7)
        lanes = jnp.bitwise_and(beyond, LANES - 1)

        def cut(x, c):
            parts = [x[c:c + 8, q * LANES:(q + 1) * LANES] for q in range(groups)]
            parts.append(jnp.concatenate(
                [x[c + 8:c + corners, q * LANES:(q + 1) * LANES] for q in range(groups)], axis=0
            ))
            return parts

        ups, lows = cut(shifts, 0), cut(lanes, 0)
        starts = [cut(values[b, c * 16:c * 16 + corners, :], 0) for c in range(3)]
        for p in range(groups + 1):
            acc = [starts[c][p] for c in range(3)]
            for k in range(reach):
                for t in range(segs):
                    mask = ups[p] == k * segs + t
                    for c in range(3):
                        row = jnp.broadcast_to(
                            ghosts[k, c:c + 1, t * LANES:(t + 1) * LANES], (8, LANES)
                        )
                        got = jnp.take_along_axis(
                            row, lows[p], axis=1, mode="promise_in_bounds"
                        )
                        acc[c] = jnp.where(mask, got, acc[c])
            for c in range(3):
                if p < groups:
                    v_ref[c * corners:c * corners + 8, p * LANES:(p + 1) * LANES] = acc[c]
                else:
                    for q in range(groups):
                        v_ref[
                            c * corners + 8:(c + 1) * corners, q * LANES:(q + 1) * LANES
                        ] = acc[c][q * rest:(q + 1) * rest]
        block_copy(b).wait()
        v = v_ref[...]
        for i in range(3 * corners):
            force = jnp.sum(blocks[b, i].astype(jnp.float32) * v, axis=0, keepdims=True)
            f_ref[i:i + 1, :] = jnp.where(b < live, force, 0.0)
        acc = None
        for a in range(corners):
            part = spread_back(
                [f_ref[c * corners + a:c * corners + a + 1, :] for c in range(3)],
                hots[b * corners + a], conn_ref[a:a + 1, at], all_height,
            )
            acc = part if acc is None else acc + part
        total[...] += acc
        return 0

    lax.fori_loop(0, steps, element_step, 0)

    def segment(c, s):
        row, lane = c * 2 * all_height + s * LANES // WIDE, s * LANES % WIDE
        return (
            total[row:row + 1, lane:lane + LANES]
            + total[row + all_height:row + all_height + 1, lane:lane + LANES]
        )

    for k in order:
        for c in range(3):
            for t in range(segs):
                back[k, c:c + 1, t * LANES:(t + 1) * LANES] = segment(
                    c, (nodes + k * bucket) // LANES + t
                )

        @pl.when(inside(k, -1))
        def _():
            back_copy(k).start()

    for k in order:

        @pl.when(inside(k, -1))
        def _():
            back_copy(k).wait_send()

        @pl.when(inside(k, 1))
        def _():
            back_copy(k).wait_recv()

    acc = None
    for k in range(reach):
        part = spread_back(
            [returned[k, c:c + 1, :] for c in range(3)], sent_hot[k], send_ref[k:k + 1, :],
            all_height,
        )
        acc = part if acc is None else acc + part
    total[...] += acc
    for c in range(3):
        for t in range(nodes // LANES):
            out_ref[c:c + 1, t * LANES:(t + 1) * LANES] = segment(c, t)


def body(field, blocks, connectivity, send_nodes, live_blocks):
    devices = lax.axis_size("dom")
    nodes = field.shape[1]
    reach2, bucket = send_nodes.shape
    reach = reach2 // 2
    offsets = [k + 1 if k < reach else reach - 1 - k for k in range(reach2)]
    corners, elements = connectivity.shape
    dofs = 3 * corners
    local_height = round_up(-(-nodes // LANES), 16)
    all_height = round_up(-(-(nodes + reach2 * bucket) // WIDE), 8)
    steps = elements // BLK
    exchanged = pltpu.VMEM((reach2, 3, bucket), jnp.float32)
    return pl.pallas_call(
        functools.partial(kernel, devices, offsets),
        out_shape=jax.ShapeDtypeStruct((3, nodes), jnp.float32),
        in_specs=[
            pl.BlockSpec(memory_space=pltpu.SMEM), VM, VM, VM,
            pl.BlockSpec(memory_space=pl.ANY),
        ],
        out_specs=VM,
        scratch_shapes=[
            pltpu.VMEM((3 * local_height, LANES), jnp.float32),
            pltpu.VMEM((3 * local_height, 2 * LANES), BF),
            exchanged, exchanged, exchanged, exchanged,
            pltpu.VMEM((reach2, LANES, bucket), BF),
            pltpu.VMEM((steps * corners, LANES, BLK), BF),
            pltpu.VMEM((steps, 48, BLK), jnp.float32),
            pltpu.VMEM((dofs, BLK), jnp.float32),
            pltpu.VMEM((dofs, BLK), jnp.float32),
            pltpu.VMEM((6 * all_height, WIDE), jnp.float32),
            pltpu.VMEM((steps, dofs, dofs, BLK), BF),
            pltpu.SemaphoreType.DMA((steps,)),
            pltpu.SemaphoreType.DMA((reach2,)),
            pltpu.SemaphoreType.DMA((reach2,)),
            pltpu.SemaphoreType.DMA((reach2,)),
            pltpu.SemaphoreType.DMA((reach2,)),
        ],
        compiler_params=pltpu.CompilerParams(collective_id=0, has_side_effects=True),
        name="stiffness",
    )(live_blocks, field, send_nodes, connectivity, blocks)


def solution(mesh):
    return jax.shard_map(
        body,
        mesh=mesh,
        in_specs=(P(None, "dom"), P(None, None, "dom"), P(None, "dom"), P(None, "dom"), P()),
        out_specs=P(None, "dom"),
        check_vma=False,
    )
```

```python
import functools

import jax
import jax.numpy as jnp
from jax import lax
from jax.experimental import pallas as pl
from jax.experimental.pallas import tpu as pltpu
from jax.sharding import PartitionSpec as P

BLK = 512
LANES = 128
WIDE = 256
SPAN = 512
LOCAL = 2
EARLY = 1
MESH = pl.DeviceIdType.MESH
VM = pl.BlockSpec(memory_space=pltpu.VMEM)
BF = jnp.bfloat16
F32 = jnp.float32


def round_up(n, m):
    return -(-n // m) * m


def split_parts(x):
    high = x.astype(BF).astype(F32)
    return high, x - high


def narrow(x):
    return x.astype(F32).astype(BF)


def lanes_of(q):
    return slice(q * LANES, (q + 1) * LANES)


def packed_row(row):
    return jnp.broadcast_to(row, (16, LANES)).astype(BF)


def merge(p, q, d):
    keep = jnp.bitwise_and(lax.broadcasted_iota(jnp.int32, p.shape, 0), d) == 0
    return jnp.where(keep, p, q) + pltpu.roll(jnp.where(keep, q, p), 8 - d, 0)


class Tree:
    def __init__(self):
        self.held = {}
        self.top = None

    def push(self, x, d=1):
        if d == 8:
            self.top = x
        elif d in self.held:
            self.push(merge(self.held.pop(d), x, d), 2 * d)
        else:
            self.held[d] = x


def index_parts(indices):
    low = jnp.bitwise_and(indices, LANES - 1).astype(F32)
    odd = jnp.bitwise_and(jnp.right_shift(indices, 7), 1).astype(F32)
    run = jnp.right_shift(indices, 8).astype(F32)
    return low, odd, run


def row_tiles(height, period):
    r = lax.broadcasted_iota(jnp.int32, (16, LANES), 0)
    tiles = []
    for t in range(0, height, 16):
        n = r + t % period
        tiles.append(narrow(jnp.where(n >= period, n - period, n)))
    return tiles


def stack(tiles):
    return jnp.concatenate(tiles, axis=0)


def pick(table, low_row, index_row, numbers, groups):
    height = table.shape[0] // 3
    columns = []
    for q in range(groups):
        low = packed_row(low_row(q))
        columns.append(stack([jnp.where(n == low, BF(1), BF(0)) for n in numbers]))
    hot = jnp.concatenate(columns, axis=1)
    spread = jnp.dot(table, stack([hot, hot]), preferred_element_type=F32)
    sub = lax.broadcasted_iota(jnp.int32, (8, LANES), 0)
    found = [[], [], []]
    for q in range(groups):
        upper = jnp.right_shift(jnp.broadcast_to(index_row(q), (8, LANES)), 7)
        acc = [jnp.zeros((8, LANES), F32) for _ in range(3)]
        for t in range(0, height, 8):
            mask = upper == sub + t
            for c in range(3):
                at = c * height + t
                acc[c] = jnp.where(mask, spread[at:at + 8, lanes_of(q)], acc[c])
        for c in range(3):
            found[c].append(acc[c])
    return [jnp.concatenate(x, axis=1) for x in found]


def spread_back(
    high_row, low_row, run_row, low_lane, odd_row, numbers, runs, groups, turned=None
):
    total = 16 * len(runs)
    height = total // 2
    zero = BF(0)
    left, right = [], []
    for q in range(groups):
        lane = packed_row(low_lane(q))
        odd = packed_row(odd_row(q))
        even = BF(1) - odd
        lower, upper = [], []
        for n in numbers:
            mask = n == lane
            lower.append(jnp.where(mask, even, zero))
            upper.append(jnp.where(mask, odd, zero))
        right.append(stack(lower + upper))
        run = packed_row(run_row(q))
        high = [packed_row(high_row(c, q)) for c in range(3)]
        low = [packed_row(low_row(c, q)) for c in range(3)]
        pieces = [[], [], []]
        for t, n in enumerate(runs):
            mask = n == run
            for c in range(3):
                if 16 * t + 16 <= height:
                    value = high[c]
                elif 16 * t >= height:
                    value = low[c]
                else:
                    split = lax.broadcasted_iota(jnp.int32, (16, LANES), 0) < height - 16 * t
                    value = jnp.where(split, high[c], low[c])
                pieces[c].append(jnp.where(mask, value, zero))
        left.append(stack(pieces[0] + pieces[1] + pieces[2]))
    if turned is None:
        return lax.dot_general(
            jnp.concatenate(left, axis=1), jnp.concatenate(right, axis=1),
            (((1,), (1,)), ((), ())), preferred_element_type=F32,
        )
    turned[...] = jnp.concatenate(right[:2], axis=1).T
    return lax.dot_general(
        jnp.concatenate(left[2:], axis=1), jnp.concatenate(right[2:], axis=1),
        (((1,), (1,)), ((), ())), preferred_element_type=F32,
    ) + jnp.dot(jnp.concatenate(left[:2], axis=1), turned[...], preferred_element_type=F32)


def kernel(
    devices, offsets, live_ref, field_hbm, send_hbm, conn_hbm, blocks_hbm, out_ref,
    field_ref, send_ref, conn_ref,
    tabf, table, outgoing, ghosts, back, returned, ret_high, ret_low, sent_parts, parts, values,
    v_ref, forces, turned, total, own_total, summed,
    blocks, in_sem, block_sem, send_sem, recv_sem, back_sem, ret_sem,
):
    me = lax.axis_index("dom")
    nodes = field_ref.shape[1]
    reach, bucket = send_ref.shape
    corners, elements = conn_ref.shape
    dofs = 3 * corners
    steps = elements // BLK
    groups = BLK // LANES
    segs = bucket // LANES
    rest = corners - 8
    local_height = table.shape[0] // 3
    all_height = total.shape[0] // 6
    own_height = own_total.shape[0] // 6

    def inside(k, sign):
        other = me + sign * offsets[k]
        return (other >= 0) & (other < devices)

    barrier = pltpu.get_barrier_semaphore()
    count = 0
    for k in range(reach):
        count = count + inside(k, 1).astype(jnp.int32)

        @pl.when(inside(k, 1))
        def _():
            pl.semaphore_signal(
                barrier, inc=1, device_id=(me + offsets[k],), device_id_type=MESH
            )

    def block_copy(b):
        return pltpu.make_async_copy(
            blocks_hbm.at[:, :, pl.ds(pl.multiple_of(b * BLK, BLK), BLK)],
            blocks.at[b],
            block_sem.at[b],
        )

    inputs = [
        pltpu.make_async_copy(source, target, in_sem.at[i])
        for i, (source, target) in enumerate(
            ((field_hbm, field_ref), (send_hbm, send_ref), (conn_hbm, conn_ref))
        )
    ]
    for copy in inputs:
        copy.start()
    inputs[0].wait()
    inputs[1].wait()

    numbers, runs = row_tiles(LANES, LANES), row_tiles(2 * all_height, all_height)
    own_runs = row_tiles(2 * own_height, own_height)

    tabf[...] = jnp.zeros_like(tabf)
    for c in range(3):
        for t in range(nodes // LANES):
            row = c * local_height + t
            tabf[row:row + 1, :] = field_ref[c:c + 1, lanes_of(t)]
    high, low = split_parts(tabf[...])
    table[:, :LANES] = high.astype(BF)
    table[:, LANES:] = low.astype(BF)

    for i, part in enumerate(index_parts(send_ref[...])):
        sent_parts[i] = part
    trees = [Tree(), Tree(), Tree()]
    for k in range(reach):
        found = pick(
            table[...], lambda q: sent_parts[0, k:k + 1, lanes_of(q)],
            lambda q: send_ref[k:k + 1, lanes_of(q)], numbers, segs,
        )
        for c in range(3):
            trees[c].push(found[c])
    for k in range(reach):
        for c in range(3):
            outgoing[k, c:c + 1, :] = trees[c].top[k:k + 1, :]

    def out_copy(k):
        return pltpu.make_async_remote_copy(
            src_ref=outgoing.at[k], dst_ref=ghosts.at[k],
            send_sem=send_sem.at[k], recv_sem=recv_sem.at[k],
            device_id=(me + offsets[k],), device_id_type=MESH,
        )

    def back_copy(k):
        return pltpu.make_async_remote_copy(
            src_ref=back.at[k], dst_ref=returned.at[k],
            send_sem=back_sem.at[k], recv_sem=ret_sem.at[k],
            device_id=(me - offsets[k],), device_id_type=MESH,
        )

    order = sorted(range(reach), key=lambda k: -abs(offsets[k]))
    for k in range(reach):

        @pl.when(jnp.logical_not(inside(k, -1)))
        def _():
            ghosts[k] = jnp.zeros(ghosts.shape[1:], F32)

        @pl.when(jnp.logical_not(inside(k, 1)))
        def _():
            returned[k] = jnp.zeros(returned.shape[1:], F32)

    inputs[2].wait()
    total[...] = jnp.zeros_like(total)

    def at_of(b, q):
        return pl.ds(pl.multiple_of(b * BLK + q * LANES, LANES), LANES)

    def local_block(b):
        at = pl.ds(pl.multiple_of(b * BLK, BLK), BLK)
        for i, part in enumerate(index_parts(conn_ref[:, at])):
            parts[b, i] = part
        trees = [Tree(), Tree(), Tree()]
        others = []
        for a in range(corners):
            found = pick(
                table[...], lambda q: parts[b, 0, a:a + 1, lanes_of(q)],
                lambda q: conn_ref[a:a + 1, at_of(b, q)], numbers, groups,
            )
            if a < 8:
                for c in range(3):
                    trees[c].push(found[c])
            else:
                others.append(found)
        for c in range(3):
            for q in range(groups):
                values[b, c * (groups + 1) + q] = trees[c].top[:, lanes_of(q)]
            tree = Tree()
            for q in range(groups):
                for found in others:
                    tree.push(found[c][:, lanes_of(q)])
            values[b, c * (groups + 1) + groups] = tree.top

    def local_step(i, _):
        @pl.when(i == EARLY)
        def _():
            pl.semaphore_wait(barrier, count)
            for k in order:

                @pl.when(inside(k, 1))
                def _():
                    out_copy(k).start()

            for n in range(steps):
                block_copy(n).start()

        for j in range(LOCAL):
            local_block(LOCAL * i + j)
        return 0

    lax.fori_loop(0, steps // LOCAL, local_step, 0)

    for k in order:

        @pl.when(inside(k, 1))
        def _():
            out_copy(k).wait_send()

        @pl.when(inside(k, -1))
        def _():
            out_copy(k).wait_recv()

    live = live_ref[me]

    def gather(b, p, to):
        if p < groups:
            beyond = conn_ref[0:8, at_of(b, p)] - nodes
        else:
            beyond = jnp.concatenate(
                [conn_ref[8:corners, at_of(b, q)] for q in range(groups)], axis=0
            ) - nodes
        upper = jnp.right_shift(beyond, 7)
        lower = jnp.bitwise_and(beyond, LANES - 1)
        acc = [values[b, c * (groups + 1) + p] for c in range(3)]
        for k in range(reach):
            for t in range(segs):
                mask = upper == k * segs + t
                for c in range(3):
                    row = jnp.broadcast_to(ghosts[k, c:c + 1, lanes_of(t)], (8, LANES))
                    got = jnp.take_along_axis(row, lower, axis=1, mode="promise_in_bounds")
                    acc[c] = jnp.where(mask, got, acc[c])
        for c in range(3):
            if p < groups:
                v_ref[to, c * corners:c * corners + 8, lanes_of(p)] = acc[c]
            else:
                for q in range(groups):
                    v_ref[to, c * corners + 8:(c + 1) * corners, lanes_of(q)] = (
                        acc[c][q * rest:(q + 1) * rest]
                    )

    def products(b, first, at):
        whole = dofs // 8 * 8
        for h in range(0, BLK, SPAN):
            lanes = slice(h, h + SPAN)
            v = v_ref[at, 0:dofs, lanes]
            tree = Tree()
            for r in range(first, first + 8):
                if r < dofs:
                    x = blocks[b, r % 3 * corners + r // 3, :, lanes].astype(F32) * v
                    tail = jnp.concatenate(
                        [x[whole:], jnp.zeros((8 - dofs + whole, SPAN), F32)], axis=0
                    )
                    x = sum((x[j:j + 8] for j in range(0, whole, 8)), tail)
                else:
                    x = jnp.zeros((8, SPAN), F32)
                tree.push(x)
            high, low = split_parts(jnp.where(b < live, tree.top, 0.0))
            forces[0, first:first + 8, lanes] = high
            forces[1, first:first + 8, lanes] = low

    def scatter(b, a):
        row = lambda part: lambda c, q: forces[part, 3 * a + c:3 * a + c + 1, lanes_of(q)]
        index = lambda i: lambda q: parts[b, i, a:a + 1, lanes_of(q)]
        return spread_back(
            row(0), row(1), index(2), index(0), index(1), numbers, runs, groups,
            turned.at[a // 2 % 2] if a % 2 else None,
        )

    def element_step(b, _):
        block_copy(b).wait()
        at = lax.rem(b, 2)
        acc = None
        done = 0
        for a in range(corners):
            while done < min(3 * a + 3, dofs):
                products(b, done, at)
                done += 8
            part = scatter(b, a)
            acc = part if acc is None else acc + part
        total[...] += acc
        for p in range(groups + 1):
            gather(jnp.minimum(b + 1, steps - 1), p, 1 - at)
        return 0

    for p in range(groups + 1):
        gather(0, p, 0)
    lax.fori_loop(0, steps, element_step, 0)

    def add_parts():
        for c in range(3):
            at = 2 * c * all_height
            summed[c * all_height:(c + 1) * all_height, :] = (
                total[at:at + all_height, :] + total[at + all_height:at + 2 * all_height, :]
            )

    def segment(c, s):
        row, lane = c * all_height + s * LANES // WIDE, s * LANES % WIDE
        return summed[row:row + 1, lane:lane + LANES]

    add_parts()
    for k in order:
        for c in range(3):
            for t in range(segs):
                back[k, c:c + 1, lanes_of(t)] = segment(c, (nodes + k * bucket) // LANES + t)

        @pl.when(inside(k, -1))
        def _():
            back_copy(k).start()

    acc = None
    for k in order:

        @pl.when(inside(k, 1))
        def _():
            back_copy(k).wait_recv()

    for k in order:
        high, low = split_parts(returned[k])
        ret_high[k] = high
        ret_low[k] = low
        part = spread_back(
            lambda c, q: ret_high[k, c:c + 1, lanes_of(q)],
            lambda c, q: ret_low[k, c:c + 1, lanes_of(q)],
            lambda q: sent_parts[2, k:k + 1, lanes_of(q)],
            lambda q: sent_parts[0, k:k + 1, lanes_of(q)],
            lambda q: sent_parts[1, k:k + 1, lanes_of(q)],
            numbers, own_runs, segs,
        )
        acc = part if acc is None else acc + part
    for k in order:

        @pl.when(inside(k, -1))
        def _():
            back_copy(k).wait_send()

    own_total[...] = acc
    for c in range(3):
        at = 2 * c * own_height
        rows = slice(c * all_height, c * all_height + own_height)
        summed[rows, :] = (
            summed[rows, :] + own_total[at:at + own_height, :]
            + own_total[at + own_height:at + 2 * own_height, :]
        )
    for c in range(3):
        for t in range(nodes // LANES):
            out_ref[c:c + 1, lanes_of(t)] = segment(c, t)


def body(field, blocks, connectivity, send_nodes, live_blocks):
    devices = lax.axis_size("dom")
    nodes = field.shape[1]
    reach2, bucket = send_nodes.shape
    reach = reach2 // 2
    offsets = [k + 1 if k < reach else reach - 1 - k for k in range(reach2)]
    corners, elements = connectivity.shape
    dofs = 3 * corners
    deep = round_up(dofs, 8)
    local_height = round_up(-(-nodes // LANES), 16)
    all_height = round_up(-(-(nodes + reach2 * bucket) // WIDE), 8)
    own_height = round_up(-(-nodes // WIDE), 8)
    steps = elements // BLK
    exchanged = pltpu.VMEM((reach2, 3, bucket), F32)
    operands = [
        pltpu.with_memory_space_constraint(x, pltpu.HBM)
        for x in (live_blocks, field, send_nodes, connectivity, blocks)
    ]
    return pl.pallas_call(
        functools.partial(kernel, devices, offsets),
        out_shape=jax.ShapeDtypeStruct((3, nodes), F32),
        in_specs=[
            pl.BlockSpec(memory_space=pltpu.SMEM),
            *[pl.BlockSpec(memory_space=pltpu.HBM)] * 4,
        ],
        out_specs=VM,
        scratch_shapes=[
            pltpu.VMEM(field.shape, F32),
            pltpu.VMEM(send_nodes.shape, jnp.int32),
            pltpu.VMEM(connectivity.shape, jnp.int32),
            pltpu.VMEM((3 * local_height, LANES), F32),
            pltpu.VMEM((3 * local_height, 2 * LANES), BF),
            exchanged, exchanged, exchanged, exchanged, exchanged, exchanged,
            pltpu.VMEM((3, reach2, bucket), F32),
            pltpu.VMEM((steps, 3, corners, BLK), F32),
            pltpu.VMEM((steps, 3 * (BLK // LANES + 1), 8, LANES), F32),
            pltpu.VMEM((2, deep, BLK), F32),
            pltpu.VMEM((2, deep, BLK), F32),
            pltpu.VMEM((2, WIDE, WIDE), BF),
            pltpu.VMEM((6 * all_height, WIDE), F32),
            pltpu.VMEM((6 * own_height, WIDE), F32),
            pltpu.VMEM((3 * all_height, WIDE), F32),
            pltpu.VMEM((steps, dofs, dofs, BLK), BF),
            pltpu.SemaphoreType.DMA((3,)),
            pltpu.SemaphoreType.DMA((steps,)),
            pltpu.SemaphoreType.DMA((reach2,)),
            pltpu.SemaphoreType.DMA((reach2,)),
            pltpu.SemaphoreType.DMA((reach2,)),
            pltpu.SemaphoreType.DMA((reach2,)),
        ],
        compiler_params=pltpu.CompilerParams(
            collective_id=0, has_side_effects=True, vmem_limit_bytes=32 << 20,
        ),
        name="stiffness",
    )(*operands)


def solution(mesh):
    return jax.shard_map(
        body,
        mesh=mesh,
        in_specs=(P(None, "dom"), P(None, None, "dom"), P(None, "dom"), P(None, "dom"), P()),
        out_specs=P(None, "dom"),
        check_vma=False,
    )
```

```python
import functools

import jax
import jax.numpy as jnp
from jax import lax
from jax.experimental import pallas as pl
from jax.experimental.pallas import tpu as pltpu
from jax.sharding import PartitionSpec as P

BLK = 512
LANES = 128
WIDE = 256
SPAN = 512
LOCAL = 2
EARLY = 1
MESH = pl.DeviceIdType.MESH
VM = pl.BlockSpec(memory_space=pltpu.VMEM)
BF = jnp.bfloat16
F32 = jnp.float32


def round_up(n, m):
    return -(-n // m) * m


def split_parts(x):
    high = x.astype(BF).astype(F32)
    return high, x - high


def narrow(x):
    return x.astype(F32).astype(BF)


def lanes_of(q):
    return slice(q * LANES, (q + 1) * LANES)


def packed_row(row):
    return jnp.broadcast_to(row, (16, LANES)).astype(BF)


def merge(p, q, d):
    keep = jnp.bitwise_and(lax.broadcasted_iota(jnp.int32, p.shape, 0), d) == 0
    return jnp.where(keep, p, q) + pltpu.roll(jnp.where(keep, q, p), 8 - d, 0)


class Tree:
    def __init__(self):
        self.held = {}
        self.top = None

    def push(self, x, d=1):
        if d == 8:
            self.top = x
        elif d in self.held:
            self.push(merge(self.held.pop(d), x, d), 2 * d)
        else:
            self.held[d] = x


def index_parts(indices):
    low = jnp.bitwise_and(indices, LANES - 1).astype(F32)
    odd = jnp.bitwise_and(jnp.right_shift(indices, 7), 1).astype(F32)
    run = jnp.right_shift(indices, 8).astype(F32)
    return low, odd, run


def row_tiles(height, period):
    r = lax.broadcasted_iota(jnp.int32, (16, LANES), 0)
    tiles = []
    for t in range(0, height, 16):
        n = r + t % period
        tiles.append(narrow(jnp.where(n >= period, n - period, n)))
    return tiles


def stack(tiles):
    return jnp.concatenate(tiles, axis=0)


def pick(table, low_row, index_row, numbers, groups):
    height = table.shape[0] // 3
    columns = []
    for q in range(groups):
        low = packed_row(low_row(q))
        columns.append(stack([jnp.where(n == low, BF(1), BF(0)) for n in numbers]))
    hot = jnp.concatenate(columns, axis=1)
    spread = jnp.dot(table, stack([hot, hot]), preferred_element_type=F32)
    sub = lax.broadcasted_iota(jnp.int32, (8, LANES), 0)
    found = [[], [], []]
    for q in range(groups):
        upper = jnp.right_shift(jnp.broadcast_to(index_row(q), (8, LANES)), 7)
        acc = [jnp.zeros((8, LANES), F32) for _ in range(3)]
        for t in range(0, height, 8):
            mask = upper == sub + t
            for c in range(3):
                at = c * height + t
                acc[c] = jnp.where(mask, spread[at:at + 8, lanes_of(q)], acc[c])
        for c in range(3):
            found[c].append(acc[c])
    return [jnp.concatenate(x, axis=1) for x in found]


def spread_back(
    high_row, low_row, run_row, low_lane, odd_row, numbers, runs, groups, turned=None, ready=None,
    only_hot=False,
):
    total = 16 * len(runs)
    height = total // 2
    zero = BF(0)
    left, right = [], []
    for q in range(groups):
        lane = packed_row(low_lane(q))
        odd = packed_row(odd_row(q))
        even = BF(1) - odd
        lower, upper = [], []
        for n in numbers:
            mask = n == lane
            lower.append(jnp.where(mask, even, zero))
            upper.append(jnp.where(mask, odd, zero))
        right.append(stack(lower + upper))
        if only_hot:
            continue
        run = packed_row(run_row(q))
        high = [packed_row(high_row(c, q)) for c in range(3)]
        low = [packed_row(low_row(c, q)) for c in range(3)]
        pieces = [[], [], []]
        for t, n in enumerate(runs):
            mask = n == run
            for c in range(3):
                if 16 * t + 16 <= height:
                    value = high[c]
                elif 16 * t >= height:
                    value = low[c]
                else:
                    split = lax.broadcasted_iota(jnp.int32, (16, LANES), 0) < height - 16 * t
                    value = jnp.where(split, high[c], low[c])
                pieces[c].append(jnp.where(mask, value, zero))
        left.append(stack(pieces[0] + pieces[1] + pieces[2]))
    if only_hot:
        return jnp.concatenate(right, axis=1).T
    if ready is not None:
        return jnp.dot(jnp.concatenate(left, axis=1), ready, preferred_element_type=F32)
    if turned is None:
        return lax.dot_general(
            jnp.concatenate(left, axis=1), jnp.concatenate(right, axis=1),
            (((1,), (1,)), ((), ())), preferred_element_type=F32,
        )
    turned[...] = jnp.concatenate(right[:2], axis=1).T
    return lax.dot_general(
        jnp.concatenate(left[2:], axis=1), jnp.concatenate(right[2:], axis=1),
        (((1,), (1,)), ((), ())), preferred_element_type=F32,
    ) + jnp.dot(jnp.concatenate(left[:2], axis=1), turned[...], preferred_element_type=F32)


def kernel(
    devices, offsets, live_ref, field_hbm, send_hbm, conn_hbm, blocks_hbm, out_ref,
    field_ref, send_ref, conn_ref,
    tabf, table, outgoing, ghosts, back, returned, ret_high, ret_low, sent_parts, parts, values,
    v_ref, forces, turned, sent_hot, total, own_total, summed,
    blocks, in_sem, block_sem, send_sem, recv_sem, back_sem, ret_sem,
):
    me = lax.axis_index("dom")
    nodes = field_ref.shape[1]
    reach, bucket = send_ref.shape
    corners, elements = conn_ref.shape
    dofs = 3 * corners
    steps = elements // BLK
    groups = BLK // LANES
    segs = bucket // LANES
    rest = corners - 8
    local_height = table.shape[0] // 3
    all_height = total.shape[0] // 6
    own_height = own_total.shape[0] // 6

    def inside(k, sign):
        other = me + sign * offsets[k]
        return (other >= 0) & (other < devices)

    barrier = pltpu.get_barrier_semaphore()
    count = 0
    for k in range(reach):
        count = count + inside(k, 1).astype(jnp.int32)

        @pl.when(inside(k, 1))
        def _():
            pl.semaphore_signal(
                barrier, inc=1, device_id=(me + offsets[k],), device_id_type=MESH
            )

    def block_copy(b):
        return pltpu.make_async_copy(
            blocks_hbm.at[:, :, pl.ds(pl.multiple_of(b * BLK, BLK), BLK)],
            blocks.at[b],
            block_sem.at[b],
        )

    inputs = [
        pltpu.make_async_copy(source, target, in_sem.at[i])
        for i, (source, target) in enumerate(
            ((field_hbm, field_ref), (send_hbm, send_ref), (conn_hbm, conn_ref))
        )
    ]
    for copy in inputs:
        copy.start()
    inputs[0].wait()
    inputs[1].wait()

    numbers, runs = row_tiles(LANES, LANES), row_tiles(2 * all_height, all_height)
    own_runs = row_tiles(2 * own_height, own_height)

    tabf[...] = jnp.zeros_like(tabf)
    for c in range(3):
        for t in range(nodes // LANES):
            row = c * local_height + t
            tabf[row:row + 1, :] = field_ref[c:c + 1, lanes_of(t)]
    high, low = split_parts(tabf[...])
    table[:, :LANES] = high.astype(BF)
    table[:, LANES:] = low.astype(BF)

    for i, part in enumerate(index_parts(send_ref[...])):
        sent_parts[i] = part
    trees = [Tree(), Tree(), Tree()]
    for k in range(reach):
        found = pick(
            table[...], lambda q: sent_parts[0, k:k + 1, lanes_of(q)],
            lambda q: send_ref[k:k + 1, lanes_of(q)], numbers, segs,
        )
        for c in range(3):
            trees[c].push(found[c])
    for k in range(reach):
        for c in range(3):
            outgoing[k, c:c + 1, :] = trees[c].top[k:k + 1, :]

    def out_copy(k):
        return pltpu.make_async_remote_copy(
            src_ref=outgoing.at[k], dst_ref=ghosts.at[k],
            send_sem=send_sem.at[k], recv_sem=recv_sem.at[k],
            device_id=(me + offsets[k],), device_id_type=MESH,
        )

    def back_copy(k):
        return pltpu.make_async_remote_copy(
            src_ref=back.at[k], dst_ref=returned.at[k],
            send_sem=back_sem.at[k], recv_sem=ret_sem.at[k],
            device_id=(me - offsets[k],), device_id_type=MESH,
        )

    order = sorted(range(reach), key=lambda k: -abs(offsets[k]))
    for k in range(reach):

        @pl.when(jnp.logical_not(inside(k, -1)))
        def _():
            ghosts[k] = jnp.zeros(ghosts.shape[1:], F32)

        @pl.when(jnp.logical_not(inside(k, 1)))
        def _():
            returned[k] = jnp.zeros(returned.shape[1:], F32)

    inputs[2].wait()
    total[...] = jnp.zeros_like(total)

    def at_of(b, q):
        return pl.ds(pl.multiple_of(b * BLK + q * LANES, LANES), LANES)

    def local_block(b):
        at = pl.ds(pl.multiple_of(b * BLK, BLK), BLK)
        for i, part in enumerate(index_parts(conn_ref[:, at])):
            parts[b, i] = part
        trees = [Tree(), Tree(), Tree()]
        others = []
        for a in range(corners):
            found = pick(
                table[...], lambda q: parts[b, 0, a:a + 1, lanes_of(q)],
                lambda q: conn_ref[a:a + 1, at_of(b, q)], numbers, groups,
            )
            if a < 8:
                for c in range(3):
                    trees[c].push(found[c])
            else:
                others.append(found)
        for c in range(3):
            for q in range(groups):
                values[b, c * (groups + 1) + q] = trees[c].top[:, lanes_of(q)]
            tree = Tree()
            for q in range(groups):
                for found in others:
                    tree.push(found[c][:, lanes_of(q)])
            values[b, c * (groups + 1) + groups] = tree.top

    def local_step(i, _):
        @pl.when(i == EARLY)
        def _():
            pl.semaphore_wait(barrier, count)
            for k in order:

                @pl.when(inside(k, 1))
                def _():
                    out_copy(k).start()

            for n in range(steps):
                block_copy(n).start()

        for j in range(LOCAL):
            local_block(LOCAL * i + j)
        return 0

    lax.fori_loop(0, steps // LOCAL, local_step, 0)

    for k in order:

        @pl.when(inside(k, 1))
        def _():
            out_copy(k).wait_send()

        @pl.when(inside(k, -1))
        def _():
            out_copy(k).wait_recv()

    live = live_ref[me]

    def gather(b, p, to):
        if p < groups:
            beyond = conn_ref[0:8, at_of(b, p)] - nodes
        else:
            beyond = jnp.concatenate(
                [conn_ref[8:corners, at_of(b, q)] for q in range(groups)], axis=0
            ) - nodes
        upper = jnp.right_shift(beyond, 7)
        lower = jnp.bitwise_and(beyond, LANES - 1)
        acc = [values[b, c * (groups + 1) + p] for c in range(3)]
        for k in range(reach):
            for t in range(segs):
                mask = upper == k * segs + t
                for c in range(3):
                    row = jnp.broadcast_to(ghosts[k, c:c + 1, lanes_of(t)], (8, LANES))
                    got = jnp.take_along_axis(row, lower, axis=1, mode="promise_in_bounds")
                    acc[c] = jnp.where(mask, got, acc[c])
        for c in range(3):
            if p < groups:
                v_ref[to, c * corners:c * corners + 8, lanes_of(p)] = acc[c]
            else:
                for q in range(groups):
                    v_ref[to, c * corners + 8:(c + 1) * corners, lanes_of(q)] = (
                        acc[c][q * rest:(q + 1) * rest]
                    )

    def products(b, first, at):
        whole = dofs // 8 * 8
        for h in range(0, BLK, SPAN):
            lanes = slice(h, h + SPAN)
            v = v_ref[at, 0:dofs, lanes]
            tree = Tree()
            for r in range(first, first + 8):
                if r < dofs:
                    x = blocks[b, r % 3 * corners + r // 3, :, lanes].astype(F32) * v
                    tail = jnp.concatenate(
                        [x[whole:], jnp.zeros((8 - dofs + whole, SPAN), F32)], axis=0
                    )
                    x = sum((x[j:j + 8] for j in range(0, whole, 8)), tail)
                else:
                    x = jnp.zeros((8, SPAN), F32)
                tree.push(x)
            high, low = split_parts(jnp.where(b < live, tree.top, 0.0))
            forces[0, first:first + 8, lanes] = high
            forces[1, first:first + 8, lanes] = low

    def scatter(b, a):
        row = lambda part: lambda c, q: forces[part, 3 * a + c:3 * a + c + 1, lanes_of(q)]
        index = lambda i: lambda q: parts[b, i, a:a + 1, lanes_of(q)]
        return spread_back(
            row(0), row(1), index(2), index(0), index(1), numbers, runs, groups,
            turned.at[a // 2 % 2] if a % 2 else None,
        )

    def element_step(b, _):
        block_copy(b).wait()
        at = lax.rem(b, 2)
        acc = None
        done = 0
        for a in range(corners):
            while done < min(3 * a + 3, dofs):
                products(b, done, at)
                done += 8
            part = scatter(b, a)
            acc = part if acc is None else acc + part
        total[...] += acc
        for p in range(groups + 1):
            gather(jnp.minimum(b + 1, steps - 1), p, 1 - at)
        return 0

    for p in range(groups + 1):
        gather(0, p, 0)
    lax.fori_loop(0, steps, element_step, 0)

    def add_parts():
        for c in range(3):
            at = 2 * c * all_height
            summed[c * all_height:(c + 1) * all_height, :] = (
                total[at:at + all_height, :] + total[at + all_height:at + 2 * all_height, :]
            )

    def segment(c, s):
        row, lane = c * all_height + s * LANES // WIDE, s * LANES % WIDE
        return summed[row:row + 1, lane:lane + LANES]

    add_parts()
    for k in order:
        for c in range(3):
            for t in range(segs):
                back[k, c:c + 1, lanes_of(t)] = segment(c, (nodes + k * bucket) // LANES + t)

        @pl.when(inside(k, -1))
        def _():
            back_copy(k).start()

    for k in range(reach):
        sent_hot[k] = spread_back(
            None, None, None,
            lambda q: sent_parts[0, k:k + 1, lanes_of(q)],
            lambda q: sent_parts[1, k:k + 1, lanes_of(q)],
            numbers, own_runs, segs, only_hot=True,
        )

    acc = None
    for k in order:

        @pl.when(inside(k, 1))
        def _():
            back_copy(k).wait_recv()

    for k in order:
        high, low = split_parts(returned[k])
        ret_high[k] = high
        ret_low[k] = low
        part = spread_back(
            lambda c, q: ret_high[k, c:c + 1, lanes_of(q)],
            lambda c, q: ret_low[k, c:c + 1, lanes_of(q)],
            lambda q: sent_parts[2, k:k + 1, lanes_of(q)],
            lambda q: sent_parts[0, k:k + 1, lanes_of(q)],
            lambda q: sent_parts[1, k:k + 1, lanes_of(q)],
            numbers, own_runs, segs, ready=sent_hot[k],
        )
        acc = part if acc is None else acc + part
    for k in order:

        @pl.when(inside(k, -1))
        def _():
            back_copy(k).wait_send()

    own_total[...] = acc
    for c in range(3):
        at = 2 * c * own_height
        rows = slice(c * all_height, c * all_height + own_height)
        summed[rows, :] = (
            summed[rows, :] + own_total[at:at + own_height, :]
            + own_total[at + own_height:at + 2 * own_height, :]
        )
    for c in range(3):
        for t in range(nodes // LANES):
            out_ref[c:c + 1, lanes_of(t)] = segment(c, t)


def body(field, blocks, connectivity, send_nodes, live_blocks):
    devices = lax.axis_size("dom")
    nodes = field.shape[1]
    reach2, bucket = send_nodes.shape
    reach = reach2 // 2
    offsets = [k + 1 if k < reach else reach - 1 - k for k in range(reach2)]
    corners, elements = connectivity.shape
    dofs = 3 * corners
    deep = round_up(dofs, 8)
    local_height = round_up(-(-nodes // LANES), 16)
    all_height = round_up(-(-(nodes + reach2 * bucket) // WIDE), 8)
    own_height = round_up(-(-nodes // WIDE), 8)
    steps = elements // BLK
    exchanged = pltpu.VMEM((reach2, 3, bucket), F32)
    operands = [
        pltpu.with_memory_space_constraint(x, pltpu.HBM)
        for x in (live_blocks, field, send_nodes, connectivity, blocks)
    ]
    return pl.pallas_call(
        functools.partial(kernel, devices, offsets),
        out_shape=jax.ShapeDtypeStruct((3, nodes), F32),
        in_specs=[
            pl.BlockSpec(memory_space=pltpu.SMEM),
            *[pl.BlockSpec(memory_space=pltpu.HBM)] * 4,
        ],
        out_specs=VM,
        scratch_shapes=[
            pltpu.VMEM(field.shape, F32),
            pltpu.VMEM(send_nodes.shape, jnp.int32),
            pltpu.VMEM(connectivity.shape, jnp.int32),
            pltpu.VMEM((3 * local_height, LANES), F32),
            pltpu.VMEM((3 * local_height, 2 * LANES), BF),
            exchanged, exchanged, exchanged, exchanged, exchanged, exchanged,
            pltpu.VMEM((3, reach2, bucket), F32),
            pltpu.VMEM((steps, 3, corners, BLK), F32),
            pltpu.VMEM((steps, 3 * (BLK // LANES + 1), 8, LANES), F32),
            pltpu.VMEM((2, deep, BLK), F32),
            pltpu.VMEM((2, deep, BLK), F32),
            pltpu.VMEM((2, WIDE, WIDE), BF),
            pltpu.VMEM((reach2, bucket, WIDE), BF),
            pltpu.VMEM((6 * all_height, WIDE), F32),
            pltpu.VMEM((6 * own_height, WIDE), F32),
            pltpu.VMEM((3 * all_height, WIDE), F32),
            pltpu.VMEM((steps, dofs, dofs, BLK), BF),
            pltpu.SemaphoreType.DMA((3,)),
            pltpu.SemaphoreType.DMA((steps,)),
            pltpu.SemaphoreType.DMA((reach2,)),
            pltpu.SemaphoreType.DMA((reach2,)),
            pltpu.SemaphoreType.DMA((reach2,)),
            pltpu.SemaphoreType.DMA((reach2,)),
        ],
        compiler_params=pltpu.CompilerParams(
            collective_id=0, has_side_effects=True, vmem_limit_bytes=32 << 20,
        ),
        name="stiffness",
    )(*operands)


def solution(mesh):
    return jax.shard_map(
        body,
        mesh=mesh,
        in_specs=(P(None, "dom"), P(None, None, "dom"), P(None, "dom"), P(None, "dom"), P()),
        out_specs=P(None, "dom"),
        check_vma=False,
    )
```
